256 devices in a mesh: rep: 4 (over x), ep: 64 (over z, y, core).
Axes of the slice: x: 4, y: 4, z: 8, core: 2. Of those that a mesh axis runs over, the one named last changes fastest.
Arguments:
- out_grad: bfloat16 [16384, 2048], P(('rep', 'ep')), may hold values from -3 to 3
- saved_hidden: bfloat16 [16384, 2, 7168], P(('rep', 'ep')), may hold values from -0.59765625 to 0.59765625
- combine: bfloat16 [16384, 2], P(('rep', 'ep')), may hold values from 0.049804688 to 1
- expert_ids: int32 [16384, 2], P(('rep', 'ep')), may hold values from 0 to 7, all different within a row; in each aligned block of 64 rows (0 to 63, 64 to 127, ...) at most 24 rows name the same one
Outputs:
- down_grad: float32 [57344, 2048], P('ep', 'rep')
The draws below stay inside these ranges and needn't reach their ends.
Inputs may be any that keep to these rules, and one draw needn't show every extreme that they name: `expert_ids`: in each aligned block of 64 rows (the rows of one device), no expert is named by more than 24 slots, a bound that some block reaches; the 2 ids of a row differ; every expert is named somewhere.
All inputs are finite; a program needn't handle non-finite values.
Results may differ from the reference program's by a relative error of at most 0.0042.
Values may be sent and summed in bfloat16 or wider, within the bound.
No kernel may reach another device: no remote copies, remote signals or barrier semaphores. Data moves between devices by JAX's collectives and lax.ppermute only.
A program may use at most 64 MiB of HBM per device.

```python
import math
import jax
import jax.numpy as jnp
import numpy as np
from jax import lax

D = 2048
FF = 7168
EXPERTS = 8
TOP = 2
TOK_DEV = 64
CAP = 24
TOKENS = 16384
N_REP = 4
N_EP = 64


def shard_levels(rng, extent, pieces, smallest, top_value):
    gain = 1.0
    for axis_at, shards_of in pieces:
        draws = jax.random.uniform(jax.random.fold_in(jax.random.fold_in(rng, 6), axis_at), (shards_of,), jnp.float32, smallest / len(pieces), top_value / len(pieces))
        gain = gain * jnp.repeat(jnp.exp(draws), extent[axis_at] // shards_of).reshape((-1,) + (1,) * (len(extent) - 1 - axis_at))
    return gain


def assign_block(rng, own, number, rows, number_of, top, limit, skew):
    order = jax.random.permutation(rng, number_of)
    packed, common = shares(number_of, rows * top, limit, skew, True), shares(number_of, rows * top, limit, skew, False)
    places = jnp.arange(number_of)

    def named(sizes, turn):
        used = int((sizes > 0).sum())
        fixed = max(1, used // 4)
        moved = fixed + (places - fixed + turn * (used - fixed)) % max(1, number_of - fixed)
        return jnp.zeros((number_of,), jnp.int32).at[order[jnp.where(places < fixed, places, moved)]].set(jnp.asarray(sizes, jnp.int32))

    sizes = jnp.where(number % 4 == 0, named(packed, number // 4), named(common, number - number // 4 - 1))
    mixed = jax.random.permutation(jax.random.fold_in(own, 3), number_of)
    donor, receiver = mixed[0:number_of // 2 * 2:2], mixed[1:number_of // 2 * 2:2]
    slack = jnp.minimum(sizes[donor] - 1, limit - sizes[receiver]) // 2
    slack = jnp.where((donor == order[0]) | (receiver == order[0]) | (sizes[receiver] == 0), 0, jnp.maximum(slack, 0))
    moved = jax.random.randint(jax.random.fold_in(own, 4), (number_of // 2,), 0, 1 << 20) % (slack + 1)
    sizes = sizes.at[donor].add(-moved).at[receiver].add(moved)
    items = jnp.searchsorted(jnp.cumsum(sizes), jnp.arange(rows * top), side="right").astype(jnp.int32)
    listing = items.reshape(top, rows).T
    listing = listing[jax.random.permutation(jax.random.fold_in(own, 1), rows)]
    turn = jax.random.randint(jax.random.fold_in(own, 2), (rows, 1), 0, top)
    return jnp.take_along_axis(listing, (jnp.arange(top)[None, :] + turn) % top, axis=1)


def shares(amount, total, bound, slope, full):
    portions = [(1 << 20) // math.isqrt(standing ** slope) + 1 for standing in range(1, amount + 1)]
    largest = bound if full else min(bound, max(-(-total // amount), total * portions[0] // sum(portions)))
    least = 1 if total - largest >= amount - 1 else 0
    holding, surplus = [largest] + [least] * (amount - 1), total - largest - least * (amount - 1)
    while surplus > 0:
        candidates = [i for i in range(1, amount) if holding[i] < largest] or [i for i in range(1, amount) if holding[i] < bound]
        pool, remaining = sum([portions[i] for i in candidates]), surplus
        for i in candidates:
            extra = min(bound - holding[i], max(1, remaining * portions[i] // pool), surplus)
            holding[i] = holding[i] + extra
            surplus = surplus - extra
    return np.array(holding)


def normal_values(own_key, shape, spread, limit, cuts=(), kind=jnp.bfloat16):
    entries = jax.random.normal(own_key, shape, jnp.float32) * spread
    if len(cuts) > 0:
        entries = shard_levels(own_key, shape, cuts, -0.22, 0.18) * entries
    return jnp.clip(entries, min=-limit, max=limit).astype(kind)


def setup_inputs(seed: int = 0) -> dict:
    streams_of = jax.random.split(jax.random.key(seed), 5)
    out_grad = normal_values(streams_of[0], (TOKENS, D), 0.5, 3.0, ((0, 256),))
    saved_hidden = normal_values(streams_of[1], (TOKENS, TOP, FF), 0.1, 0.59765625, ((0, 256),))
    combine = jnp.clip(jnp.exp(math.log(1.0) - 2.9996462 * jax.random.uniform(streams_of[2], (TOKENS, TOP), jnp.float32) ** shard_levels(streams_of[2], (TOKENS, TOP), ((0, 256),), -0.2, 0.2)), 0.049804688, 1.0).astype(jnp.bfloat16)
    expert_ids_keys = jax.random.split(jax.random.fold_in(streams_of[3], 1), TOKENS // TOK_DEV)
    expert_ids_turns = jax.random.permutation(jax.random.fold_in(streams_of[3], 3), TOKENS // TOK_DEV)
    expert_ids = jax.vmap(lambda own, number: assign_block(jax.random.fold_in(streams_of[3], 2), own, number, TOK_DEV, EXPERTS, TOP, CAP, 2))(expert_ids_keys, expert_ids_turns).reshape((TOKENS, TOP))
    return {"out_grad": out_grad, "saved_hidden": saved_hidden, "combine": combine, "expert_ids": expert_ids}


def reference(out_grad, saved_hidden, combine, expert_ids):
    tok_count = out_grad.shape[0]
    slot_count = tok_count * TOP
    most_rows = N_REP * N_EP * CAP
    flat_ids = expert_ids.reshape(slot_count).astype(jnp.int32)
    flat_prob = combine.reshape(slot_count).astype(jnp.float32)
    flat_hidden = saved_hidden.reshape(slot_count, FF)
    order = jnp.argsort(flat_ids, stable=True).astype(jnp.int32)
    onehot = (flat_ids[:, None] == jnp.arange(EXPERTS, dtype=jnp.int32)[None, :]).astype(jnp.int32)
    counts = jnp.sum(onehot, axis=0).astype(jnp.int32)
    starts = (jnp.cumsum(counts) - counts).astype(jnp.int32)
    padded_order = jnp.concatenate([order, jnp.zeros((most_rows,), jnp.int32)])

    def one_expert(expert):
        chosen = lax.dynamic_slice_in_dim(padded_order, starts[expert], most_rows).astype(jnp.int32)
        valid = jnp.arange(most_rows, dtype=jnp.int32) < counts[expert]
        grad_rows = out_grad[chosen // TOP]
        prob = jnp.where(valid, flat_prob[chosen], jnp.float32(0.0))
        hidden = flat_hidden[chosen]
        scaled = (prob[:, None] * grad_rows.astype(jnp.float32)).astype(jnp.bfloat16)
        return lax.dot_general(hidden, scaled, (((0,), (0,)), ((), ())), preferred_element_type=jnp.float32)

    wgrad_all = lax.map(one_expert, jnp.arange(EXPERTS, dtype=jnp.int32))
    return wgrad_all.reshape(EXPERTS * FF, out_grad.shape[1])
```

```python
import functools

import jax
import jax.numpy as jnp
from jax import lax
from jax.experimental import pallas as pl
from jax.experimental.pallas import tpu as pltpu
from jax.sharding import Mesh, PartitionSpec as P

EXPERTS = 8
CAP = 24
CHUNKS = (384, 256, 256)
VMEM = pl.BlockSpec(memory_space=pltpu.VMEM)


def place_matrices(ids_ref):
    ids = ids_ref[...]
    tokens = ids.shape[1]
    experts = lax.broadcasted_iota(jnp.int32, (EXPERTS, tokens), 0)
    first = (ids[0:1, :] == experts).astype(jnp.float32)
    second = (ids[1:2, :] == experts).astype(jnp.float32)
    before = (
        lax.broadcasted_iota(jnp.int32, (tokens, tokens), 0)
        < lax.broadcasted_iota(jnp.int32, (tokens, tokens), 1)
    ).astype(jnp.float32)
    ahead_first = jnp.dot(first, before, preferred_element_type=jnp.float32)
    ahead_second = jnp.dot(second, before, preferred_element_type=jnp.float32)
    ahead_second = ahead_second + jnp.sum(first, axis=1, keepdims=True)
    place_first = jnp.sum(first * ahead_first, axis=0, keepdims=True).astype(jnp.int32)
    place_second = jnp.sum(second * ahead_second, axis=0, keepdims=True).astype(jnp.int32)
    rows = lax.broadcasted_iota(jnp.int32, (EXPERTS * CAP, tokens), 0)
    return (
        rows == ids[0:1, :] * CAP + place_first,
        rows == ids[1:2, :] * CAP + place_second,
    )


def pack_grad_kernel(ids_ref, prob_ref, grad_ref, out_ref):
    first, second = place_matrices(ids_ref)
    prob = prob_ref[...].astype(jnp.float32)
    pick = jnp.where(first, prob[0:1, :], 0.0) + jnp.where(second, prob[1:2, :], 0.0)
    packed = jnp.dot(
        pick.astype(jnp.bfloat16), grad_ref[...], preferred_element_type=jnp.float32
    )
    out_ref[...] = packed.astype(jnp.bfloat16).reshape(out_ref.shape)


def pack_hidden_kernel(chunks, ids_ref, hidden_ref, *out_refs):
    first, second = place_matrices(ids_ref)
    first = jnp.where(first, 1.0, 0.0).astype(jnp.bfloat16)
    second = jnp.where(second, 1.0, 0.0).astype(jnp.bfloat16)
    unit_cols = sum(chunks)
    start = 0
    for width, out_ref in zip(chunks, out_refs):
        for c in range(2):
            for y in range(4):
                at = (y * 2 + c) * unit_cols + start
                packed = jnp.dot(
                    first, hidden_ref[:, 0, at : at + width], preferred_element_type=jnp.float32
                ) + jnp.dot(
                    second, hidden_ref[:, 1, at : at + width], preferred_element_type=jnp.float32
                )
                out_ref[c * 4 + y] = packed.astype(jnp.bfloat16).reshape(EXPERTS, CAP, width)
        start += width


def per_device(out_grad, saved_hidden, combine, expert_ids):
    tok_count, model_width = out_grad.shape
    ids_t, prob_t = expert_ids.T, combine.T
    send_grad = pl.pallas_call(
        pack_grad_kernel,
        out_shape=jax.ShapeDtypeStruct((EXPERTS, CAP, model_width), jnp.bfloat16),
        in_specs=[VMEM] * 3,
        out_specs=VMEM,
    )(ids_t, prob_t, out_grad)
    send_hidden = pl.pallas_call(
        functools.partial(pack_hidden_kernel, CHUNKS),
        out_shape=[
            jax.ShapeDtypeStruct((8, EXPERTS, CAP, width), jnp.bfloat16) for width in CHUNKS
        ],
        in_specs=[VMEM] * 2,
        out_specs=[VMEM] * len(CHUNKS),
    )(ids_t, saved_hidden)

    exchange = functools.partial(lax.all_to_all, split_axis=0, concat_axis=0, tiled=True)
    by_z = exchange(send_grad, "z")
    by_y = exchange(jnp.broadcast_to(by_z[None], (4, *by_z.shape)), "y")
    by_core = exchange(jnp.broadcast_to(by_y[None], (2, *by_y.shape)), "core")
    grad_rows = by_core.reshape(-1, model_width)
    contract_rows = (((0,), (0,)), ((), ()))
    pieces = []
    for width, piece in zip(CHUNKS, send_hidden):
        arrived = exchange(piece.reshape(64, CAP, width), ("core", "y", "z"))
        hidden_rows = arrived.reshape(-1, width)
        part = lax.dot_general(
            hidden_rows, grad_rows, contract_rows, preferred_element_type=jnp.float32
        ).astype(jnp.bfloat16)
        part = jnp.moveaxis(part.reshape(width, 4, model_width // 4), 1, 0)
        pieces.append(exchange(part, "rep").astype(jnp.float32).sum(axis=0))
    return jnp.concatenate(pieces, axis=0)


def solution(mesh):
    wide = Mesh(mesh.devices.reshape(4, 8, 4, 2), ("rep", "z", "y", "core"))
    rows = ("rep", "z", "y", "core")
    in_specs = (P(rows, None), P(rows, None, None), P(rows, None), P(rows, None))
    out_specs = P(("z", "y", "core"), "rep")
    return jax.shard_map(
        per_device, mesh=wide, in_specs=in_specs, out_specs=out_specs, check_vma=False
    )
```

```python
import functools

import jax
import jax.numpy as jnp
from jax import lax
from jax.experimental import pallas as pl
from jax.experimental.pallas import tpu as pltpu
from jax.sharding import Mesh, PartitionSpec as P

EXPERTS = 8
CAP = 24
CHUNKS = (896,)
VMEM = pl.BlockSpec(memory_space=pltpu.VMEM)
SMEM = pl.BlockSpec(memory_space=pltpu.SMEM)
PIECES = tuple(
    (flip, d, low, high)
    for flip in range(2)
    for d, low, high in ((0, 0, 8), (1, 0, 4), (1, 4, 8), (3, 0, 4), (3, 4, 8), (2, 0, 4), (2, 4, 8))
)
BLOCKS = (2, 1, 3, 0)


def cost(flops, moved):
    return pl.CostEstimate(flops=flops, bytes_accessed=moved, transcendentals=0)


def place_matrices(ids):
    tokens = ids.shape[1]
    experts = lax.broadcasted_iota(jnp.int32, (EXPERTS, tokens), 0)
    first = (ids[0:1, :] == experts).astype(jnp.float32)
    second = (ids[1:2, :] == experts).astype(jnp.float32)
    before = (
        lax.broadcasted_iota(jnp.int32, (tokens, tokens), 0)
        < lax.broadcasted_iota(jnp.int32, (tokens, tokens), 1)
    ).astype(jnp.float32)
    ahead_first = jnp.dot(first, before, preferred_element_type=jnp.float32)
    ahead_second = jnp.dot(second, before, preferred_element_type=jnp.float32)
    ahead_second = ahead_second + jnp.sum(first, axis=1, keepdims=True)
    place_first = jnp.sum(first * ahead_first, axis=0, keepdims=True).astype(jnp.int32)
    place_second = jnp.sum(second * ahead_second, axis=0, keepdims=True).astype(jnp.int32)
    rows = lax.broadcasted_iota(jnp.int32, (EXPERTS * CAP, tokens), 0)
    return (
        rows == ids[0:1, :] * CAP + place_first,
        rows == ids[1:2, :] * CAP + place_second,
    )


def pack_grad_kernel(at_ref, ids_ref, prob_ref, grad_ref, out_ref):
    first, second = place_matrices(ids_ref[...])
    prob = prob_ref[...].astype(jnp.float32)
    pick = jnp.where(first, prob[0:1, :], 0.0) + jnp.where(second, prob[1:2, :], 0.0)
    pick = pick.astype(jnp.bfloat16)
    cols = grad_ref.shape[1] // 4
    for k in range(4):
        owner = lax.rem(at_ref[0] + BLOCKS[k], 4)
        block = grad_ref[:, pl.ds(pl.multiple_of(owner * cols, cols), cols)]
        packed = jnp.dot(pick, block, preferred_element_type=jnp.float32).astype(jnp.bfloat16)
        out_ref[:, :, k * cols : (k + 1) * cols] = packed.reshape(EXPERTS, CAP, cols)


def pack_hidden_kernel(chunks, ids_ref, hidden_ref, *out_refs):
    first, second = place_matrices(ids_ref[...])
    first = jnp.where(first, 1.0, 0.0).astype(jnp.bfloat16)
    second = jnp.where(second, 1.0, 0.0).astype(jnp.bfloat16)
    unit_cols = sum(chunks)
    start = 0
    for width, out_ref in zip(chunks, out_refs):
        for c in range(2):
            for y in range(4):
                at = (y * 2 + c) * unit_cols + start
                packed = jnp.dot(
                    first, hidden_ref[:, 0, at : at + width], preferred_element_type=jnp.float32
                ) + jnp.dot(
                    second, hidden_ref[:, 1, at : at + width], preferred_element_type=jnp.float32
                )
                out_ref[c * 4 + y] = packed.astype(jnp.bfloat16).reshape(EXPERTS, CAP, width)
        start += width


def product_kernel(blocks, at_ref, hidden_hbm, *refs):
    piece_hbm, out_refs = refs[: len(PIECES)], refs[len(PIECES) : -3]
    hidden, grad, sems = refs[-3:]
    y, core = at_ref[2], at_ref[3]
    block = hidden.shape[0] // 8
    cols = grad.shape[1] // len(blocks)
    copies = []
    for flip in range(2):
        for d in range(4):
            r = flip * 4 + d
            source = lax.rem(core + flip, 2) * 4 + lax.rem(y + (4 - d), 4)
            rows = pl.ds(pl.multiple_of(source * block, block), block)
            here = hidden.at[r * block : (r + 1) * block]
            copies.append(pltpu.make_async_copy(hidden_hbm.at[rows], here, sems.at[0, r]))
    first = min(blocks) * cols
    for n, (flip, d, low, high) in enumerate(PIECES):
        start = (flip * 4 + d) * block
        here = grad.at[start + low * CAP : start + high * CAP]
        there = piece_hbm[n].at[:, first : first + len(blocks) * cols]
        copies.append(pltpu.make_async_copy(there, here, sems.at[1, n]))
    for copy in copies:
        copy.start()
    for copy in copies:
        copy.wait()
    half = hidden.shape[1] // 2
    outs = list(out_refs)
    for k in blocks:
        at = k * cols - first
        part = lax.dot_general(
            hidden[...],
            grad[:, at : at + cols],
            (((0,), (0,)), ((), ())),
            preferred_element_type=jnp.float32,
        )
        if k == 3:
            outs.pop(0)[...] = part
        else:
            low, high = outs.pop(0), outs.pop(0)
            low[...] = part[:half].astype(low.dtype)
            high[...] = part[half:].astype(high.dtype)


def shifted(array, axis, by):
    n = lax.axis_size(axis)
    return lax.ppermute(array, axis, [(i, (i + by) % n) for i in range(n)])


def per_device(out_grad, saved_hidden, combine, expert_ids):
    tok_count, model_width = out_grad.shape
    unit_cols = saved_hidden.shape[2] // 8
    ids_t, prob_t = expert_ids.T, combine.T
    at = jnp.stack([lax.axis_index(name) for name in ("rep", "z", "y", "core")]).astype(jnp.int32)
    exchange = functools.partial(lax.all_to_all, split_axis=0, concat_axis=0, tiled=True)

    send_grad = pl.pallas_call(
        pack_grad_kernel,
        out_shape=jax.ShapeDtypeStruct((EXPERTS, CAP, model_width), jnp.bfloat16),
        in_specs=[SMEM] + [VMEM] * 3,
        out_specs=VMEM,
        cost_estimate=cost(2 * 192 * 64 * 2048, 1 << 20),
    )(at, ids_t, prob_t, out_grad)
    own = exchange(send_grad, "z")

    send_hidden = pl.pallas_call(
        functools.partial(pack_hidden_kernel, CHUNKS),
        out_shape=[
            jax.ShapeDtypeStruct((8, EXPERTS, CAP, width), jnp.bfloat16) for width in CHUNKS
        ],
        in_specs=[VMEM] * 2,
        out_specs=[VMEM] * len(CHUNKS),
        cost_estimate=cost(2 * 192 * 128 * 7168, 5 << 20),
    )(ids_t, saved_hidden)

    half = EXPERTS // 2
    own_low, own_high = own[:half], own[half:]
    behind_low, ahead_high = shifted(own_low, "y", 1), shifted(own_high, "y", 3)
    behind_high, ahead_low = shifted(own_high, "y", 1), shifted(own_low, "y", 3)
    far_low, far_high = shifted(behind_low, "y", 1), shifted(ahead_high, "y", 3)
    near = [own, behind_low, behind_high, ahead_low, ahead_high, far_low, far_high]
    other = [lax.ppermute(piece, "core", [(0, 1), (1, 0)]) for piece in near]
    pieces = [piece.reshape(-1, model_width) for piece in near + other]

    cols = model_width // 4
    hbm = pl.BlockSpec(memory_space=pltpu.HBM)
    done = []
    arrived = None
    for width, packed in zip(CHUNKS, send_hidden):
        if arrived is not None:
            packed, arrived = lax.optimization_barrier((packed, arrived))
        arrived = exchange(packed.reshape(64, CAP, width), ("core", "y", "z"))
        narrow = jax.ShapeDtypeStruct((width // 2, cols), jnp.bfloat16)
        wide = jax.ShapeDtypeStruct((width // 2, cols), jnp.float32)

        def product(blocks, outs):
            return pl.pallas_call(
                functools.partial(product_kernel, blocks),
                out_shape=outs,
                in_specs=[SMEM] + [hbm] * (1 + len(PIECES)),
                out_specs=[VMEM] * len(outs),
                scratch_shapes=[
                    pltpu.VMEM((64 * CAP, width), jnp.bfloat16),
                    pltpu.VMEM((64 * CAP, len(blocks) * cols), jnp.bfloat16),
                    pltpu.SemaphoreType.DMA((2, len(PIECES))),
                ],
                cost_estimate=cost(2 * 1536 * width * cols * len(blocks), 4 << 20),
            )(at, arrived.reshape(-1, width), *pieces)

        far_a, far_b = product((0,), [narrow] * 2)
        right_a, right_b, left_a, left_b, own_part = product(
            (1, 2, 3),
            [wide, narrow, narrow, wide, jax.ShapeDtypeStruct((width, cols), jnp.float32)],
        )
        from_left = shifted(far_a, "rep", 1)
        from_right = shifted(far_b, "rep", 3)
        low = shifted(left_a, "rep", 3)
        high = shifted(right_b, "rep", 1)
        right_a = (right_a + from_left.astype(jnp.float32)).astype(jnp.bfloat16)
        left_b = (left_b + from_right.astype(jnp.float32)).astype(jnp.bfloat16)
        low = low.astype(jnp.float32) + shifted(right_a, "rep", 1).astype(jnp.float32)
        high = high.astype(jnp.float32) + shifted(left_b, "rep", 3).astype(jnp.float32)
        done.append(own_part + jnp.concatenate([low, high], axis=0))
    return jnp.concatenate(done, axis=0)


def solution(mesh):
    wide = Mesh(mesh.devices.reshape(4, 8, 4, 2), ("rep", "z", "y", "core"))
    rows = ("rep", "z", "y", "core")
    in_specs = (P(rows, None), P(rows, None, None), P(rows, None), P(rows, None))
    out_specs = P(("z", "y", "core"), "rep")
    return jax.shard_map(
        per_device, mesh=wide, in_specs=in_specs, out_specs=out_specs, check_vma=False
    )
```

```python
import functools

import jax
import jax.numpy as jnp
from jax import lax
from jax.experimental import pallas as pl
from jax.experimental.pallas import tpu as pltpu
from jax.sharding import Mesh, PartitionSpec as P

EXPERTS = 8
CAP = 24
DIRECT = 512
FAR_FIRST = (4, 3, 5, 2, 6, 1, 7)
VMEM = pl.BlockSpec(memory_space=pltpu.VMEM)
SMEM = pl.BlockSpec(memory_space=pltpu.SMEM)
PIECES = tuple(
    (flip, d, low, high)
    for flip in range(2)
    for d, low, high in ((0, 0, 8), (1, 0, 8), (3, 0, 8), (2, 0, 4), (2, 4, 8))
)
BLOCKS = (2, 1, 3, 0)


def cost(flops, moved):
    return pl.CostEstimate(flops=flops, bytes_accessed=moved, transcendentals=0)


def place_matrices(ids):
    tokens = ids.shape[1]
    experts = lax.broadcasted_iota(jnp.int32, (EXPERTS, tokens), 0)
    first = (ids[0:1, :] == experts).astype(jnp.float32)
    second = (ids[1:2, :] == experts).astype(jnp.float32)
    before = (
        lax.broadcasted_iota(jnp.int32, (tokens, tokens), 0)
        < lax.broadcasted_iota(jnp.int32, (tokens, tokens), 1)
    ).astype(jnp.float32)
    ahead_first = jnp.dot(first, before, preferred_element_type=jnp.float32)
    ahead_second = jnp.dot(second, before, preferred_element_type=jnp.float32)
    ahead_second = ahead_second + jnp.sum(first, axis=1, keepdims=True)
    place_first = jnp.sum(first * ahead_first, axis=0, keepdims=True).astype(jnp.int32)
    place_second = jnp.sum(second * ahead_second, axis=0, keepdims=True).astype(jnp.int32)
    rows = lax.broadcasted_iota(jnp.int32, (EXPERTS * CAP, tokens), 0)
    return (
        rows == ids[0:1, :] * CAP + place_first,
        rows == ids[1:2, :] * CAP + place_second,
    )


def pack_grad_kernel(at_ref, ids_ref, prob_ref, grad_ref, out_ref):
    first, second = place_matrices(ids_ref[...])
    prob = prob_ref[...].astype(jnp.float32)
    pick = jnp.where(first, prob[0:1, :], 0.0) + jnp.where(second, prob[1:2, :], 0.0)
    pick = pick.astype(jnp.bfloat16)
    cols = grad_ref.shape[1] // 4
    for k in range(4):
        owner = lax.rem(at_ref[0] + BLOCKS[k], 4)
        block = grad_ref[:, pl.ds(pl.multiple_of(owner * cols, cols), cols)]
        packed = jnp.dot(pick, block, preferred_element_type=jnp.float32).astype(jnp.bfloat16)
        out_ref[:, :, k * cols : (k + 1) * cols] = packed.reshape(EXPERTS, CAP, cols)


def pack_hidden_kernel(unit_cols, ids_ref, hidden_ref, out_ref):
    first, second = place_matrices(ids_ref[...])
    first = jnp.where(first, 1.0, 0.0).astype(jnp.bfloat16)
    second = jnp.where(second, 1.0, 0.0).astype(jnp.bfloat16)
    width = out_ref.shape[3]

    def pack(n, carry):
        owner = lax.rem(n, 4) * 2 + lax.div(n, 4)
        cols = pl.ds(pl.multiple_of(owner * unit_cols, 128), width)
        packed = jnp.dot(
            first, hidden_ref[:, 0, cols], preferred_element_type=jnp.float32
        ) + jnp.dot(second, hidden_ref[:, 1, cols], preferred_element_type=jnp.float32)
        out_ref[n] = packed.astype(jnp.bfloat16).reshape(EXPERTS, CAP, width)
        return carry

    lax.fori_loop(0, 8, pack, 0)


def pack_rest_kernel(unit_cols, at_ref, ids_ref, hidden_ref, *out_refs):
    first, second = place_matrices(lax.rem(ids_ref[...] + (EXPERTS - at_ref[1]), EXPERTS))
    first = jnp.where(first, 1.0, 0.0).astype(jnp.bfloat16)
    second = jnp.where(second, 1.0, 0.0).astype(jnp.bfloat16)
    width = out_refs[0].shape[3]
    for d in range(4):

        def pack(flip, carry, d=d):
            owner = lax.rem(at_ref[2] + d, 4) * 2 + lax.rem(at_ref[3] + flip, 2)
            cols = pl.ds(pl.multiple_of(owner * unit_cols + (unit_cols - width), 128), width)
            packed = jnp.dot(
                first, hidden_ref[:, 0, cols], preferred_element_type=jnp.float32
            ) + jnp.dot(second, hidden_ref[:, 1, cols], preferred_element_type=jnp.float32)
            out_refs[d][flip] = packed.astype(jnp.bfloat16).reshape(EXPERTS, CAP, width)
            return carry

        lax.fori_loop(0, 2, pack, 0)


def for_other_core_kernel(*refs):
    *in_refs, out_ref = refs
    for d in range(4):
        out_ref[d] = in_refs[d][...]


def regroup_kernel(*refs):
    ours, theirs, out_refs = refs[:4], refs[4], refs[5:]
    for s in range(EXPERTS):
        for d in range(4):
            out_refs[s][d] = ours[d][s]
            out_refs[s][4 + d] = theirs[d, s]


def product_kernel(blocks, at_ref, *refs):
    grad, sems = refs[-2:]
    direct = len(refs[0].shape) == 2
    hidden_refs, refs = (refs[:1], refs[1:-2]) if direct else (refs[:EXPERTS], refs[EXPERTS:-2])
    piece_hbm, out_refs = refs[: len(PIECES)], refs[len(PIECES) :]
    z, y, core = at_ref[1], at_ref[2], at_ref[3]
    block = grad.shape[0] // 8
    cols = grad.shape[1] // len(blocks)
    copies = []
    sources = [
        lax.rem(core + flip, 2) * 4 + lax.rem(y + (4 - d), 4)
        for flip in range(2)
        for d in range(4)
    ]
    first = min(blocks) * cols
    for n, (flip, d, low, high) in enumerate(PIECES):
        start = pl.multiple_of(sources[flip * 4 + d] * block + low * CAP, 4 * CAP)
        here = grad.at[pl.ds(start, (high - low) * CAP)]
        there = piece_hbm[n].at[:, first : first + len(blocks) * cols]
        copies.append(pltpu.make_async_copy(there, here, sems.at[n]))
    for copy in copies:
        copy.start()
    for copy in copies:
        copy.wait()
    if direct:
        hidden = hidden_refs[0][...]
    else:
        sorted_rows, out_refs = out_refs[-1], out_refs[:-1]
        for s in range(EXPERTS):
            plane = lax.rem(z + (EXPERTS - s), EXPERTS)
            for r in range(8):
                sorted_rows[sources[r] * EXPERTS + plane] = hidden_refs[s][r]
        hidden = sorted_rows[...].reshape(grad.shape[0], -1)
    half = hidden.shape[1] // 2
    outs = list(out_refs)
    for k in blocks:
        at = k * cols - first
        part = lax.dot_general(
            hidden,
            grad[:, at : at + cols],
            (((0,), (0,)), ((), ())),
            preferred_element_type=jnp.float32,
        )
        if k == 0:
            outs[0][...] = part[:half].astype(jnp.bfloat16)
            outs[1][...] = part[half:].astype(jnp.bfloat16)
        else:
            outs.pop(0)[...] = part


def shifted(array, axis, by):
    n = lax.axis_size(axis)
    return lax.ppermute(array, axis, [(i, (i + by) % n) for i in range(n)])


def other_core(array):
    return lax.ppermute(array, "core", [(0, 1), (1, 0)])


def per_device(out_grad, saved_hidden, combine, expert_ids):
    _, model_width = out_grad.shape
    unit_cols = saved_hidden.shape[2] // 8
    rest = unit_cols - DIRECT
    ids_t, prob_t = expert_ids.T, combine.T
    at = jnp.stack([lax.axis_index(name) for name in ("rep", "z", "y", "core")]).astype(jnp.int32)
    exchange = functools.partial(lax.all_to_all, split_axis=0, concat_axis=0, tiled=True)

    send_grad = pl.pallas_call(
        pack_grad_kernel,
        out_shape=jax.ShapeDtypeStruct((EXPERTS, CAP, model_width), jnp.bfloat16),
        in_specs=[SMEM] + [VMEM] * 3,
        out_specs=VMEM,
        cost_estimate=cost(2 * 192 * 64 * 2048, 1 << 20),
    )(at, ids_t, prob_t, out_grad)
    own = exchange(send_grad, "z")

    plane_rows = pl.pallas_call(
        functools.partial(pack_rest_kernel, unit_cols),
        out_shape=[jax.ShapeDtypeStruct((2, EXPERTS, CAP, rest), jnp.bfloat16)] * 4,
        in_specs=[SMEM] + [VMEM] * 2,
        out_specs=[VMEM] * 4,
        cost_estimate=cost(2 * 192 * 128 * rest * 8, 4 << 20),
    )(at, ids_t, saved_hidden)
    plane_rows = [plane_rows[0]] + [shifted(plane_rows[d], "y", d) for d in (1, 2, 3)]
    part = (None, EXPERTS, CAP, rest)
    ours = pl.BlockSpec(part, lambda i: (0, 0, 0, 0))
    theirs = pl.BlockSpec(part, lambda i: (1, 0, 0, 0))
    for_other = pl.pallas_call(
        for_other_core_kernel,
        grid=(1,),
        out_shape=jax.ShapeDtypeStruct((4, EXPERTS, CAP, rest), jnp.bfloat16),
        in_specs=[theirs] * 4,
        out_specs=pl.BlockSpec((4, EXPERTS, CAP, rest), lambda i: (0, 0, 0, 0)),
        cost_estimate=cost(0, 3 << 20),
    )(*plane_rows)
    rest_to = pl.pallas_call(
        regroup_kernel,
        grid=(1,),
        out_shape=[jax.ShapeDtypeStruct((8, CAP, rest), jnp.bfloat16)] * EXPERTS,
        in_specs=[ours] * 4 + [pl.BlockSpec((4, EXPERTS, CAP, rest), lambda i: (0, 0, 0, 0))],
        out_specs=[pl.BlockSpec((8, CAP, rest), lambda i: (0, 0, 0))] * EXPERTS,
        cost_estimate=cost(0, 5 << 20),
    )(*plane_rows, other_core(for_other))

    send_hidden = pl.pallas_call(
        functools.partial(pack_hidden_kernel, unit_cols),
        out_shape=jax.ShapeDtypeStruct((8, EXPERTS, CAP, DIRECT), jnp.bfloat16),
        in_specs=[VMEM] * 2,
        out_specs=VMEM,
        cost_estimate=cost(2 * 192 * 128 * DIRECT * 8, 4 << 20),
    )(ids_t, saved_hidden)
    arrived = exchange(send_hidden.reshape(64, CAP, DIRECT), ("core", "y", "z"))

    half = EXPERTS // 2
    behind, ahead = shifted(own, "y", 1), shifted(own, "y", 3)
    far_low, far_high = shifted(behind[:half], "y", 1), shifted(ahead[half:], "y", 3)
    near = [own, behind, ahead, far_low, far_high]
    pieces = [piece.reshape(-1, model_width) for piece in near + [other_core(p) for p in near]]
    rest_from = [rest_to[0]] + [None] * 7
    for s in FAR_FIRST:
        rest_from[s] = shifted(rest_to[s], "z", s)

    cols = model_width // 4
    hbm = pl.BlockSpec(memory_space=pltpu.HBM)

    def partial_sums(width, hidden):
        narrow = jax.ShapeDtypeStruct((width // 2, cols), jnp.bfloat16)
        sort_space = [] if len(hidden) == 1 else [pltpu.VMEM((64, CAP, width), jnp.bfloat16)]

        def product(blocks, outs):
            return pl.pallas_call(
                functools.partial(product_kernel, blocks),
                out_shape=outs,
                in_specs=[SMEM] + [VMEM] * len(hidden) + [hbm] * len(PIECES),
                out_specs=[VMEM] * len(outs),
                scratch_shapes=sort_space
                + [
                    pltpu.VMEM((64 * CAP, len(blocks) * cols), jnp.bfloat16),
                    pltpu.SemaphoreType.DMA((len(PIECES),)),
                ],
                cost_estimate=cost(2 * 1536 * width * cols * len(blocks), 4 << 20),
            )(at, *hidden, *pieces)

        far = product((0,), [narrow] * 2)
        near = product((1, 2, 3), [jax.ShapeDtypeStruct((width, cols), jnp.float32)] * 3)
        return far, near

    def exchanged(far, near):
        right, left, own_part = near
        rows = own_part.shape[0] // 2
        from_left, from_right = shifted(far[0], "rep", 1), shifted(far[1], "rep", 3)
        from_left, from_right = from_left.astype(jnp.float32), from_right.astype(jnp.float32)
        right = (right + jnp.pad(from_left, ((0, rows), (0, 0)))).astype(jnp.bfloat16)
        left = (left + jnp.pad(from_right, ((rows, 0), (0, 0)))).astype(jnp.bfloat16)
        return own_part, shifted(right, "rep", 1), shifted(left, "rep", 3)

    def summed(own_part, from_left, from_right):
        return own_part + from_left.astype(jnp.float32) + from_right.astype(jnp.float32)

    direct = exchanged(*partial_sums(DIRECT, [arrived.reshape(-1, DIRECT)]))
    other = exchanged(*partial_sums(rest, rest_from))
    return jnp.concatenate([summed(*direct), summed(*other)], axis=0)


def solution(mesh):
    wide = Mesh(mesh.devices.reshape(4, 8, 4, 2), ("rep", "z", "y", "core"))
    rows = ("rep", "z", "y", "core")
    in_specs = (P(rows, None), P(rows, None, None), P(rows, None), P(rows, None))
    out_specs = P(("z", "y", "core"), "rep")
    return jax.shard_map(
        per_device, mesh=wide, in_specs=in_specs, out_specs=out_specs, check_vma=False
    )
```

```python
import functools

import jax
import jax.numpy as jnp
from jax import lax
from jax.experimental import pallas as pl
from jax.experimental.pallas import tpu as pltpu
from jax.sharding import Mesh, PartitionSpec as P

EXPERTS = 8
CAP = 24
DIRECT = 384
FAR_FIRST = (4, 3, 5, 2, 6, 1, 7)
VMEM = pl.BlockSpec(memory_space=pltpu.VMEM)
SMEM = pl.BlockSpec(memory_space=pltpu.SMEM)
EARLY = ((0, 0, 0), (0, 1, 0), (0, 3, 0), (1, 0, 0), (1, 1, 0), (1, 3, 0))
LATE = ((0, 2, 0), (0, 2, 4), (1, 2, 0), (1, 2, 4))
BLOCKS = (2, 1, 3, 0)


def cost(flops, moved):
    return pl.CostEstimate(flops=flops, bytes_accessed=moved, transcendentals=0)


def place_matrices(ids):
    tokens = ids.shape[1]
    experts = lax.broadcasted_iota(jnp.int32, (EXPERTS, tokens), 0)
    first = (ids[0:1, :] == experts).astype(jnp.float32)
    second = (ids[1:2, :] == experts).astype(jnp.float32)
    before = (
        lax.broadcasted_iota(jnp.int32, (tokens, tokens), 0)
        < lax.broadcasted_iota(jnp.int32, (tokens, tokens), 1)
    ).astype(jnp.float32)
    ahead_first = jnp.dot(first, before, preferred_element_type=jnp.float32)
    ahead_second = jnp.dot(second, before, preferred_element_type=jnp.float32)
    ahead_second = ahead_second + jnp.sum(first, axis=1, keepdims=True)
    place_first = jnp.sum(first * ahead_first, axis=0, keepdims=True).astype(jnp.int32)
    place_second = jnp.sum(second * ahead_second, axis=0, keepdims=True).astype(jnp.int32)
    rows = lax.broadcasted_iota(jnp.int32, (EXPERTS * CAP, tokens), 0)
    return (
        rows == ids[0:1, :] * CAP + place_first,
        rows == ids[1:2, :] * CAP + place_second,
    )


def pack_grad_kernel(at_ref, ids_ref, prob_ref, grad_ref, out_ref):
    first, second = place_matrices(ids_ref[...])
    prob = prob_ref[...].astype(jnp.float32)
    pick = jnp.where(first, prob[0:1, :], 0.0) + jnp.where(second, prob[1:2, :], 0.0)
    pick = pick.astype(jnp.bfloat16)
    cols = grad_ref.shape[1] // 4
    for k in range(4):
        owner = lax.rem(at_ref[0] + BLOCKS[k], 4)
        block = grad_ref[:, pl.ds(pl.multiple_of(owner * cols, cols), cols)]
        packed = jnp.dot(pick, block, preferred_element_type=jnp.float32).astype(jnp.bfloat16)
        out_ref[:, :, k * cols : (k + 1) * cols] = packed.reshape(EXPERTS, CAP, cols)


def pack_hidden_kernel(unit_cols, ids_ref, hidden_ref, out_ref):
    first, second = place_matrices(ids_ref[...])
    first = jnp.where(first, 1.0, 0.0).astype(jnp.bfloat16)
    second = jnp.where(second, 1.0, 0.0).astype(jnp.bfloat16)
    width = out_ref.shape[3]

    def pack(n, carry):
        owner = lax.rem(n, 4) * 2 + lax.div(n, 4)
        cols = pl.ds(pl.multiple_of(owner * unit_cols, 128), width)
        packed = jnp.dot(
            first, hidden_ref[:, 0, cols], preferred_element_type=jnp.float32
        ) + jnp.dot(second, hidden_ref[:, 1, cols], preferred_element_type=jnp.float32)
        out_ref[n] = packed.astype(jnp.bfloat16).reshape(EXPERTS, CAP, width)
        return carry

    lax.fori_loop(0, 8, pack, 0)


def pack_rest_kernel(unit_cols, at_ref, ids_ref, hidden_ref, *out_refs):
    first, second = place_matrices(lax.rem(ids_ref[...] + (EXPERTS - at_ref[1]), EXPERTS))
    first = jnp.where(first, 1.0, 0.0).astype(jnp.bfloat16)
    second = jnp.where(second, 1.0, 0.0).astype(jnp.bfloat16)
    width = out_refs[0].shape[3]
    for d in range(4):

        def pack(flip, carry, d=d):
            owner = lax.rem(at_ref[2] + d, 4) * 2 + lax.rem(at_ref[3] + flip, 2)
            cols = pl.ds(pl.multiple_of(owner * unit_cols + (unit_cols - width), 128), width)
            packed = jnp.dot(
                first, hidden_ref[:, 0, cols], preferred_element_type=jnp.float32
            ) + jnp.dot(second, hidden_ref[:, 1, cols], preferred_element_type=jnp.float32)
            out_refs[d][flip] = packed.astype(jnp.bfloat16).reshape(EXPERTS, CAP, width)
            return carry

        lax.fori_loop(0, 2, pack, 0)


def for_other_core_kernel(*refs):
    *in_refs, out_ref = refs
    for d in range(4):
        out_ref[d] = in_refs[d][...]


def regroup_kernel(*refs):
    ours, theirs, out_refs = refs[:4], refs[4], refs[5:]
    for s in range(EXPERTS):
        for d in range(4):
            out_refs[s][d] = ours[d][s]
            out_refs[s][4 + d] = theirs[d, s]


def put_kernel(pieces, at_ref, *refs):
    piece_refs, (out_ref, sems) = refs[len(refs) - 2 - len(pieces) : -2], refs[-2:]
    block = out_ref.shape[0] // 8
    copies = []
    for n, (flip, d, low) in enumerate(pieces):
        source = lax.rem(at_ref[3] + flip, 2) * 4 + lax.rem(at_ref[2] + (4 - d), 4)
        start = pl.multiple_of(source * block + low * CAP, 4 * CAP)
        rows = out_ref.at[pl.ds(start, piece_refs[n].shape[0])]
        copies.append(pltpu.make_async_copy(piece_refs[n], rows, sems.at[n]))
    for copy in copies:
        copy.start()
    for copy in copies:
        copy.wait()


def sort_rows_kernel(at_ref, *refs):
    *in_refs, out_ref = refs
    for flip in range(2):
        for d in range(4):
            source = lax.rem(at_ref[3] + flip, 2) * 4 + lax.rem(at_ref[2] + (4 - d), 4)
            for s in range(EXPERTS):
                plane = lax.rem(at_ref[1] + (EXPERTS - s), EXPERTS)
                out_ref[source * EXPERTS + plane] = in_refs[s][flip * 4 + d]


def shifted(array, axis, by):
    n = lax.axis_size(axis)
    return lax.ppermute(array, axis, [(i, (i + by) % n) for i in range(n)])


def other_core(array):
    return lax.ppermute(array, "core", [(0, 1), (1, 0)])


def per_device(out_grad, saved_hidden, combine, expert_ids):
    _, model_width = out_grad.shape
    unit_cols = saved_hidden.shape[2] // 8
    rest = unit_cols - DIRECT
    ids_t, prob_t = expert_ids.T, combine.T
    at = jnp.stack([lax.axis_index(name) for name in ("rep", "z", "y", "core")]).astype(jnp.int32)
    exchange = functools.partial(lax.all_to_all, split_axis=0, concat_axis=0, tiled=True)

    send_grad = pl.pallas_call(
        pack_grad_kernel,
        out_shape=jax.ShapeDtypeStruct((EXPERTS, CAP, model_width), jnp.bfloat16),
        in_specs=[SMEM] + [VMEM] * 3,
        out_specs=VMEM,
        cost_estimate=cost(2 * 192 * 64 * 2048, 1 << 20),
    )(at, ids_t, prob_t, out_grad)
    own = exchange(send_grad, "z")

    plane_rows = pl.pallas_call(
        functools.partial(pack_rest_kernel, unit_cols),
        out_shape=[jax.ShapeDtypeStruct((2, EXPERTS, CAP, rest), jnp.bfloat16)] * 4,
        in_specs=[SMEM] + [VMEM] * 2,
        out_specs=[VMEM] * 4,
        cost_estimate=cost(2 * 192 * 128 * rest * 8, 4 << 20),
    )(at, ids_t, saved_hidden)
    plane_rows = [plane_rows[0]] + [shifted(plane_rows[d], "y", d) for d in (1, 2, 3)]
    part = (None, EXPERTS, CAP, rest)
    ours = pl.BlockSpec(part, lambda i: (0, 0, 0, 0))
    theirs = pl.BlockSpec(part, lambda i: (1, 0, 0, 0))
    for_other = pl.pallas_call(
        for_other_core_kernel,
        grid=(1,),
        out_shape=jax.ShapeDtypeStruct((4, EXPERTS, CAP, rest), jnp.bfloat16),
        in_specs=[theirs] * 4,
        out_specs=pl.BlockSpec((4, EXPERTS, CAP, rest), lambda i: (0, 0, 0, 0)),
        cost_estimate=cost(0, 3 << 20),
    )(*plane_rows)
    rest_to = pl.pallas_call(
        regroup_kernel,
        grid=(1,),
        out_shape=[jax.ShapeDtypeStruct((8, CAP, rest), jnp.bfloat16)] * EXPERTS,
        in_specs=[ours] * 4 + [pl.BlockSpec((4, EXPERTS, CAP, rest), lambda i: (0, 0, 0, 0))],
        out_specs=[pl.BlockSpec((8, CAP, rest), lambda i: (0, 0, 0))] * EXPERTS,
        cost_estimate=cost(0, 5 << 20),
    )(*plane_rows, other_core(for_other))

    send_hidden = pl.pallas_call(
        functools.partial(pack_hidden_kernel, unit_cols),
        out_shape=jax.ShapeDtypeStruct((8, EXPERTS, CAP, DIRECT), jnp.bfloat16),
        in_specs=[VMEM] * 2,
        out_specs=VMEM,
        cost_estimate=cost(2 * 192 * 128 * DIRECT * 8, 4 << 20),
    )(ids_t, saved_hidden)
    arrived = exchange(send_hidden.reshape(64, CAP, DIRECT), ("core", "y", "z"))

    half = EXPERTS // 2
    behind, ahead = shifted(own, "y", 1), shifted(own, "y", 3)
    far_low, far_high = shifted(behind[:half], "y", 1), shifted(ahead[half:], "y", 3)
    flat = [piece.reshape(-1, model_width) for piece in (own, behind, ahead, far_low, far_high)]
    theirs = [other_core(piece) for piece in flat]
    rest_from = [rest_to[0]] + [None] * 7
    for s in FAR_FIRST:
        rest_from[s] = shifted(rest_to[s], "z", s)

    cols = model_width // 4
    hbm = pl.BlockSpec(memory_space=pltpu.HBM)
    whole = jax.ShapeDtypeStruct((64 * CAP, model_width), jnp.bfloat16)
    grad_rows = pl.pallas_call(
        functools.partial(put_kernel, EARLY),
        out_shape=whole,
        in_specs=[SMEM] + [VMEM] * len(EARLY),
        out_specs=hbm,
        scratch_shapes=[pltpu.SemaphoreType.DMA((len(EARLY),))],
        cost_estimate=cost(0, 9 << 20),
    )(at, *flat[:3], *theirs[:3])
    grad_rows = pl.pallas_call(
        functools.partial(put_kernel, LATE),
        out_shape=whole,
        in_specs=[SMEM, hbm] + [VMEM] * len(LATE),
        out_specs=hbm,
        scratch_shapes=[pltpu.SemaphoreType.DMA((len(LATE),))],
        input_output_aliases={1: 0},
        cost_estimate=cost(0, 3 << 20),
    )(at, grad_rows, *flat[3:], *theirs[3:])

    def product(hidden, start, stop):
        return lax.dot_general(
            hidden,
            grad_rows[:, start:stop],
            (((0,), (0,)), ((), ())),
            preferred_element_type=jnp.float32,
        )

    def partial_sums(hidden):
        half = hidden.shape[1] // 2
        far = product(hidden, 0, cols).astype(jnp.bfloat16)
        far = [far[:half], far[half:]]
        near = product(hidden, cols, 4 * cols)
        return far, near

    def exchanged(far, near):
        right, left, own_part = (near[:, k * cols : (k + 1) * cols] for k in range(3))
        half = near.shape[0] // 2
        from_left, from_right = shifted(far[0], "rep", 1), shifted(far[1], "rep", 3)
        from_left, from_right = from_left.astype(jnp.float32), from_right.astype(jnp.float32)
        right = (right + jnp.pad(from_left, ((0, half), (0, 0)))).astype(jnp.bfloat16)
        left = (left + jnp.pad(from_right, ((half, 0), (0, 0)))).astype(jnp.bfloat16)
        return own_part, shifted(right, "rep", 1), shifted(left, "rep", 3)

    def summed(own_part, from_left, from_right):
        return own_part + from_left.astype(jnp.float32) + from_right.astype(jnp.float32)

    direct = exchanged(*partial_sums(arrived.reshape(-1, DIRECT)))
    rest_rows = pl.pallas_call(
        sort_rows_kernel,
        out_shape=jax.ShapeDtypeStruct((64, CAP, rest), jnp.bfloat16),
        in_specs=[SMEM] + [VMEM] * EXPERTS,
        out_specs=VMEM,
        cost_estimate=cost(0, 3 << 20),
    )(at, *rest_from)
    other = exchanged(*partial_sums(rest_rows.reshape(-1, rest)))
    return jnp.concatenate([summed(*direct), summed(*other)], axis=0)


def solution(mesh):
    wide = Mesh(mesh.devices.reshape(4, 8, 4, 2), ("rep", "z", "y", "core"))
    rows = ("rep", "z", "y", "core")
    in_specs = (P(rows, None), P(rows, None, None), P(rows, None), P(rows, None))
    out_specs = P(("z", "y", "core"), "rep")
    return jax.shard_map(
        per_device, mesh=wide, in_specs=in_specs, out_specs=out_specs, check_vma=False
    )
```

```python
import functools

import jax
import jax.numpy as jnp
from jax import lax
from jax.experimental import pallas as pl
from jax.experimental.pallas import tpu as pltpu
from jax.sharding import Mesh, PartitionSpec as P

EXPERTS = 8
CAP = 24
DIRECT = 384
FAR_FIRST = (4, 3, 5, 2, 6, 1, 7)
VMEM = pl.BlockSpec(memory_space=pltpu.VMEM)
SMEM = pl.BlockSpec(memory_space=pltpu.SMEM)
EARLY = ((0, 0, 0), (0, 1, 0), (0, 3, 0), (1, 0, 0), (1, 1, 0), (1, 3, 0))
LATE = ((0, 2, 0), (0, 2, 4), (1, 2, 0), (1, 2, 4))
BLOCKS = (2, 1, 3, 0)


def cost(flops, moved):
    return pl.CostEstimate(flops=flops, bytes_accessed=moved, transcendentals=0)


def place_matrices(ids):
    tokens = ids.shape[1]
    experts = lax.broadcasted_iota(jnp.int32, (EXPERTS, tokens), 0)
    first = (ids[0:1, :] == experts).astype(jnp.float32)
    second = (ids[1:2, :] == experts).astype(jnp.float32)
    before = (
        lax.broadcasted_iota(jnp.int32, (tokens, tokens), 0)
        < lax.broadcasted_iota(jnp.int32, (tokens, tokens), 1)
    ).astype(jnp.float32)
    ahead_first = jnp.dot(first, before, preferred_element_type=jnp.float32)
    ahead_second = jnp.dot(second, before, preferred_element_type=jnp.float32)
    ahead_second = ahead_second + jnp.sum(first, axis=1, keepdims=True)
    place_first = jnp.sum(first * ahead_first, axis=0, keepdims=True).astype(jnp.int32)
    place_second = jnp.sum(second * ahead_second, axis=0, keepdims=True).astype(jnp.int32)
    rows = lax.broadcasted_iota(jnp.int32, (EXPERTS * CAP, tokens), 0)
    return (
        rows == ids[0:1, :] * CAP + place_first,
        rows == ids[1:2, :] * CAP + place_second,
    )


def pack_grad_kernel(ids_ref, prob_ref, grad_ref, out_ref):
    first, second = place_matrices(ids_ref[...])
    prob = prob_ref[...].astype(jnp.float32)
    pick = jnp.where(first, prob[0:1, :], 0.0) + jnp.where(second, prob[1:2, :], 0.0)
    pick = pick.astype(jnp.bfloat16)
    cols = grad_ref.shape[1] // 4
    for k in range(4):
        owner = lax.rem(lax.axis_index("rep") + BLOCKS[k], 4)
        block = grad_ref[:, pl.ds(pl.multiple_of(owner * cols, cols), cols)]
        packed = jnp.dot(pick, block, preferred_element_type=jnp.float32).astype(jnp.bfloat16)
        out_ref[:, :, k * cols : (k + 1) * cols] = packed.reshape(EXPERTS, CAP, cols)


def pack_hidden_kernel(unit_cols, ids_ref, hidden_ref, out_ref):
    first, second = place_matrices(ids_ref[...])
    first = jnp.where(first, 1.0, 0.0).astype(jnp.bfloat16)
    second = jnp.where(second, 1.0, 0.0).astype(jnp.bfloat16)
    width = out_ref.shape[3]

    def pack(n, carry):
        owner = lax.rem(n, 4) * 2 + lax.div(n, 4)
        cols = pl.ds(pl.multiple_of(owner * unit_cols, 128), width)
        packed = jnp.dot(
            first, hidden_ref[:, 0, cols], preferred_element_type=jnp.float32
        ) + jnp.dot(second, hidden_ref[:, 1, cols], preferred_element_type=jnp.float32)
        out_ref[n] = packed.astype(jnp.bfloat16).reshape(EXPERTS, CAP, width)
        return carry

    lax.fori_loop(0, 8, pack, 0)


def pack_rest_kernel(unit_cols, at_ref, ids_ref, hidden_ref, *out_refs):
    first, second = place_matrices(lax.rem(ids_ref[...] + (EXPERTS - at_ref[1]), EXPERTS))
    first = jnp.where(first, 1.0, 0.0).astype(jnp.bfloat16)
    second = jnp.where(second, 1.0, 0.0).astype(jnp.bfloat16)
    width = out_refs[0].shape[3]
    for d in range(4):

        def pack(flip, carry, d=d):
            owner = lax.rem(at_ref[2] + d, 4) * 2 + lax.rem(at_ref[3] + flip, 2)
            cols = pl.ds(pl.multiple_of(owner * unit_cols + (unit_cols - width), 128), width)
            packed = jnp.dot(
                first, hidden_ref[:, 0, cols], preferred_element_type=jnp.float32
            ) + jnp.dot(second, hidden_ref[:, 1, cols], preferred_element_type=jnp.float32)
            out_refs[d][flip] = packed.astype(jnp.bfloat16).reshape(EXPERTS, CAP, width)
            return carry

        lax.fori_loop(0, 2, pack, 0)


def for_other_core_kernel(*refs):
    *in_refs, out_ref = refs
    for d in range(4):
        out_ref[d] = in_refs[d][...]


def regroup_kernel(*refs):
    ours, theirs, out_refs = refs[:4], refs[4], refs[5:]
    for s in range(EXPERTS):
        for d in range(4):
            out_refs[s][d] = ours[d][s]
            out_refs[s][4 + d] = theirs[d, s]


def put_kernel(pieces, at_ref, *refs):
    piece_refs, (out_ref, sems) = refs[len(refs) - 2 - len(pieces) : -2], refs[-2:]
    block = out_ref.shape[0] // 8
    copies = []
    for n, (flip, d, low) in enumerate(pieces):
        source = lax.rem(at_ref[3] + flip, 2) * 4 + lax.rem(at_ref[2] + (4 - d), 4)
        start = pl.multiple_of(source * block + low * CAP, 4 * CAP)
        rows = out_ref.at[pl.ds(start, piece_refs[n].shape[0])]
        copies.append(pltpu.make_async_copy(piece_refs[n], rows, sems.at[n]))
    for copy in copies:
        copy.start()
    for copy in copies:
        copy.wait()


def sort_rows_kernel(at_ref, *refs):
    *in_refs, out_ref = refs
    for flip in range(2):
        for d in range(4):
            source = lax.rem(at_ref[3] + flip, 2) * 4 + lax.rem(at_ref[2] + (4 - d), 4)
            for s in range(EXPERTS):
                plane = lax.rem(at_ref[1] + (EXPERTS - s), EXPERTS)
                out_ref[source * EXPERTS + plane] = in_refs[s][flip * 4 + d]


def shifted(array, axis, by):
    n = lax.axis_size(axis)
    return lax.ppermute(array, axis, [(i, (i + by) % n) for i in range(n)])


def other_core(array):
    return lax.ppermute(array, "core", [(0, 1), (1, 0)])


def per_device(out_grad, saved_hidden, combine, expert_ids):
    _, model_width = out_grad.shape
    unit_cols = saved_hidden.shape[2] // 8
    rest = unit_cols - DIRECT
    ids_t, prob_t = expert_ids.T, combine.T
    at = jnp.stack([lax.axis_index(name) for name in ("rep", "z", "y", "core")]).astype(jnp.int32)
    exchange = functools.partial(lax.all_to_all, split_axis=0, concat_axis=0, tiled=True)

    send_grad = pl.pallas_call(
        pack_grad_kernel,
        out_shape=jax.ShapeDtypeStruct((EXPERTS, CAP, model_width), jnp.bfloat16),
        in_specs=[VMEM] * 3,
        out_specs=VMEM,
        cost_estimate=cost(2 * 192 * 64 * 2048, 1 << 20),
    )(ids_t, prob_t, out_grad)
    own = exchange(send_grad, "z")

    plane_rows = pl.pallas_call(
        functools.partial(pack_rest_kernel, unit_cols),
        out_shape=[jax.ShapeDtypeStruct((2, EXPERTS, CAP, rest), jnp.bfloat16)] * 4,
        in_specs=[SMEM] + [VMEM] * 2,
        out_specs=[VMEM] * 4,
        cost_estimate=cost(2 * 192 * 128 * rest * 8, 4 << 20),
    )(at, ids_t, saved_hidden)
    plane_rows = [plane_rows[0]] + [shifted(plane_rows[d], "y", d) for d in (1, 2, 3)]
    part = (None, EXPERTS, CAP, rest)
    ours = pl.BlockSpec(part, lambda i: (0, 0, 0, 0))
    theirs = pl.BlockSpec(part, lambda i: (1, 0, 0, 0))
    for_other = pl.pallas_call(
        for_other_core_kernel,
        grid=(1,),
        out_shape=jax.ShapeDtypeStruct((4, EXPERTS, CAP, rest), jnp.bfloat16),
        in_specs=[theirs] * 4,
        out_specs=pl.BlockSpec((4, EXPERTS, CAP, rest), lambda i: (0, 0, 0, 0)),
        cost_estimate=cost(0, 3 << 20),
    )(*plane_rows)
    rest_to = pl.pallas_call(
        regroup_kernel,
        grid=(1,),
        out_shape=[jax.ShapeDtypeStruct((8, CAP, rest), jnp.bfloat16)] * EXPERTS,
        in_specs=[ours] * 4 + [pl.BlockSpec((4, EXPERTS, CAP, rest), lambda i: (0, 0, 0, 0))],
        out_specs=[pl.BlockSpec((8, CAP, rest), lambda i: (0, 0, 0))] * EXPERTS,
        cost_estimate=cost(0, 5 << 20),
    )(*plane_rows, other_core(for_other))

    send_hidden = pl.pallas_call(
        functools.partial(pack_hidden_kernel, unit_cols),
        out_shape=jax.ShapeDtypeStruct((8, EXPERTS, CAP, DIRECT), jnp.bfloat16),
        in_specs=[VMEM] * 2,
        out_specs=VMEM,
        cost_estimate=cost(2 * 192 * 128 * DIRECT * 8, 4 << 20),
    )(ids_t, saved_hidden)
    arrived = exchange(send_hidden.reshape(64, CAP, DIRECT), ("core", "y", "z"))

    half = EXPERTS // 2
    behind = shifted(own, "y", 1)
    ahead = shifted(own, "y", 3)
    far_low, far_high = shifted(behind[:half], "y", 1), shifted(ahead[half:], "y", 3)
    flat = [piece.reshape(-1, model_width) for piece in (own, behind, ahead, far_low, far_high)]
    theirs = [other_core(piece) for piece in flat]
    rest_from = [rest_to[0]] + [None] * 7
    for s in FAR_FIRST:
        rest_from[s] = shifted(rest_to[s], "z", s)

    cols = model_width // 4
    hbm = pl.BlockSpec(memory_space=pltpu.HBM)
    whole = jax.ShapeDtypeStruct((64 * CAP, model_width), jnp.bfloat16)
    grad_rows = pl.pallas_call(
        functools.partial(put_kernel, EARLY),
        out_shape=whole,
        in_specs=[SMEM] + [VMEM] * len(EARLY),
        out_specs=hbm,
        scratch_shapes=[pltpu.SemaphoreType.DMA((len(EARLY),))],
        cost_estimate=cost(0, 9 << 20),
    )(at, *flat[:3], *theirs[:3])
    grad_rows = pl.pallas_call(
        functools.partial(put_kernel, LATE),
        out_shape=whole,
        in_specs=[SMEM, hbm] + [VMEM] * len(LATE),
        out_specs=hbm,
        scratch_shapes=[pltpu.SemaphoreType.DMA((len(LATE),))],
        input_output_aliases={1: 0},
        cost_estimate=cost(0, 3 << 20),
    )(at, grad_rows, *flat[3:], *theirs[3:])

    def product(hidden, start, stop):
        return lax.dot_general(
            hidden,
            grad_rows[:, start:stop],
            (((0,), (0,)), ((), ())),
            preferred_element_type=jnp.float32,
        )

    def partial_sums(hidden):
        half = hidden.shape[1] // 2
        far = product(hidden, 0, cols).astype(jnp.bfloat16)
        far = [far[:half], far[half:]]
        near = product(hidden, cols, 4 * cols)
        return far, near

    def exchanged(far, near):
        right, left, own_part = (near[:, k * cols : (k + 1) * cols] for k in range(3))
        half = near.shape[0] // 2
        from_left, from_right = shifted(far[0], "rep", 1), shifted(far[1], "rep", 3)
        from_left, from_right = from_left.astype(jnp.float32), from_right.astype(jnp.float32)
        right = (right + jnp.pad(from_left, ((0, half), (0, 0)))).astype(jnp.bfloat16)
        left = (left + jnp.pad(from_right, ((half, 0), (0, 0)))).astype(jnp.bfloat16)
        return own_part, shifted(right, "rep", 1), shifted(left, "rep", 3)

    def summed(own_part, from_left, from_right):
        return own_part + from_left.astype(jnp.float32) + from_right.astype(jnp.float32)

    direct = exchanged(*partial_sums(arrived.reshape(-1, DIRECT)))
    rest_rows = pl.pallas_call(
        sort_rows_kernel,
        out_shape=jax.ShapeDtypeStruct((64, CAP, rest), jnp.bfloat16),
        in_specs=[SMEM] + [VMEM] * EXPERTS,
        out_specs=VMEM,
        cost_estimate=cost(0, 3 << 20),
    )(at, *rest_from)
    other = exchanged(*partial_sums(rest_rows.reshape(-1, rest)))
    first_rows = jnp.pad(summed(*direct), ((0, rest), (0, 0)))
    return lax.dynamic_update_slice(first_rows, summed(*other), (DIRECT, 0))


def solution(mesh):
    wide = Mesh(mesh.devices.reshape(4, 8, 4, 2), ("rep", "z", "y", "core"))
    rows = ("rep", "z", "y", "core")
    in_specs = (P(rows, None), P(rows, None, None), P(rows, None), P(rows, None))
    out_specs = P(("z", "y", "core"), "rep")
    return jax.shard_map(
        per_device, mesh=wide, in_specs=in_specs, out_specs=out_specs, check_vma=False
    )
```
